256 devices in a mesh: row: 32 (over z, x), col: 8 (over y, core).
Axes of the slice: x: 4, y: 4, z: 8, core: 2. Of those that a mesh axis runs over, the one named last changes fastest.
Arguments:
- factor: float32 [9, 1024, 3, 1024], P(None, 'row', None, 'col'), may hold values from -2 to 2.5, as said below
- adjoint: float32 [9, 1024, 3, 1024], P(None, 'row', None, 'col'), may hold values from -6 to 6
Outputs:
- kernel_adjoint: float32 [9, 1024, 3, 1024], P(None, 'row', None, 'col')
The draws below stay inside these ranges and needn't reach their ends.
Inputs may be any that keep to these rules, and one draw needn't show every extreme that they name: `factor`: zero where the column minus 2048 exceeds the row; the diagonal entries of the two 512-square diagonal blocks lie between 1 and 2.5.
All inputs are finite; a program needn't handle non-finite values.
Results may differ from the reference program's by a relative error of at most 0.0001.
Values sent between devices are 32-bit elements; how exact they have to be, the bound alone decides.
No kernel may reach another device: no remote copies, remote signals or barrier semaphores. Data moves between devices by JAX's collectives and lax.ppermute only.
A program may use at most 64 MiB of HBM per device.

```python
import jax
import jax.numpy as jnp
from jax import lax

NB = 512
RC = 9
CC = 3
RW = 1024
CW = 1024
NR = 9216
NC = 3072
LEFT = 2048


def draw_factor(key, part):
    key_base = jax.random.fold_in(key, 11)
    key_diag = jax.random.fold_in(key, 12)
    raw_draw = jnp.clip(jax.random.normal(key_base, (NR, NC), jnp.float32), -6.0, 6.0)
    diag_values = jax.random.uniform(key_diag, (NR, 1), jnp.float32, 1.0, 2.0)
    row_ids = jnp.arange(NR, dtype=jnp.int32)[:, None]
    col_ids = jnp.arange(NC, dtype=jnp.int32)[None, :] - LEFT
    panel_rows = row_ids < 2 * NB
    scale_map = jnp.where(panel_rows, NB ** (-0.5), NR ** (-0.5))
    same_block = (col_ids >= 0) & (col_ids // NB == row_ids // NB) & panel_rows
    scale_map = jnp.where(same_block, 0.4 * NB ** (-0.5), scale_map)
    values = raw_draw * scale_map
    values = jnp.where(same_block & (col_ids == row_ids), diag_values, values)
    values = jnp.where(col_ids > row_ids, 0.0, values)
    return values.reshape(RC, RW, CC, CW)


def steps_of(key, dims, pieces, least, high):
    factor_of, own = 1.0, jax.random.fold_in(key, 6)
    for dim, blocks in pieces:
        steps = jnp.exp(jax.random.uniform(jax.random.fold_in(own, dim), (blocks,), jnp.float32, least / len(pieces), high / len(pieces)))
        factor_of = factor_of * jnp.repeat(steps, dims[dim] // blocks).reshape([-1 if axis == dim else 1 for axis in range(len(dims))])
    return factor_of


def bell_draw(rng, shape, scale, limit, pieces=(), held_as=jnp.bfloat16):
    result = scale * jax.random.normal(rng, shape, jnp.float32)
    if pieces:
        result = result * steps_of(rng, shape, pieces, -0.22, 0.18)
    return jnp.clip(result, -limit, limit).astype(held_as)


def setup_inputs(seed: int = 0) -> dict:
    streams_of = jax.random.split(jax.random.key(seed), 3)
    return {
        "factor": draw_factor(jax.random.fold_in(streams_of[2], 71), 0),
        "adjoint": bell_draw(streams_of[1], (RC, RW, CC, CW), 1.0, 6.0, ((1, 32), (3, 8)), jnp.float32),
    }


def exact_dot(first, second):
    return jnp.dot(first.astype(jnp.float32), second.astype(jnp.float32), precision=lax.Precision.HIGHEST, preferred_element_type=jnp.float32)

def lower_half(matrix):
    return jnp.tril(matrix) - 0.5 * jnp.diag(jnp.diag(matrix))

def reference(factor, adjoint):
    factor_mat = factor.reshape(NR, NC)
    row_ids = jnp.arange(NR, dtype=jnp.int32)[:, None]
    col_ids = jnp.arange(NC, dtype=jnp.int32)[None, :]
    working = jnp.where(col_ids - LEFT > row_ids, 0.0, adjoint.reshape(NR, NC))
    for panel_index in (1,):
        first_row = panel_index * NB
        bottom = first_row + NB
        first_col = LEFT + first_row
        last_col = first_col + NB
        diag_block = factor_mat[first_row:bottom, first_col:last_col]
        row_block = factor_mat[first_row:bottom, :first_col]
        trail_block = factor_mat[bottom:, :first_col]
        panel_block = factor_mat[bottom:, first_col:last_col]
        column_adjoint = lax.linalg.triangular_solve(diag_block, working[bottom:, first_col:last_col], left_side=False, lower=True)
        trail_adjoint = working[bottom:, :first_col] - exact_dot(column_adjoint, row_block)
        diag_start = working[first_row:bottom, first_col:last_col] - jnp.tril(exact_dot(column_adjoint.T, panel_block))
        product = lower_half(exact_dot(diag_block.T, diag_start))
        left_solved = lax.linalg.triangular_solve(diag_block, product, left_side=True, lower=True, transpose_a=True)
        symmetric = lax.linalg.triangular_solve(diag_block, left_solved, left_side=False, lower=True)
        diag_adjoint = lower_half(symmetric + symmetric.T)
        row_adjoint = working[first_row:bottom, :first_col] - exact_dot(column_adjoint.T, trail_block) - exact_dot(diag_adjoint + diag_adjoint.T, row_block)
        working = working.at[bottom:, first_col:last_col].set(column_adjoint)
        working = working.at[bottom:, :first_col].set(trail_adjoint)
        working = working.at[first_row:bottom, first_col:last_col].set(diag_adjoint)
        working = working.at[first_row:bottom, :first_col].set(row_adjoint)
    return working.reshape(RC, RW, CC, CW)
```

```python
import jax
import jax.numpy as jnp
from jax import lax
from jax.experimental import pallas as pl
from jax.experimental.pallas import tpu as pltpu
from jax.sharding import Mesh
from jax.sharding import PartitionSpec as P

NB = 512
TILE = 128
ROW = ("z", "x")


def exact_dot(first, second, over=((1,), (0,))):
    return lax.dot_general(
        first, second, (over, ((), ())),
        precision=lax.Precision.HIGHEST, preferred_element_type=jnp.float32,
    )


def inverse_kernel(diag_ref, inv_ref):
    rows = lax.broadcasted_iota(jnp.int32, (TILE, TILE), 0)
    cols = lax.broadcasted_iota(jnp.int32, (TILE, TILE), 1)
    blocks = NB // TILE
    eye = rows == cols
    diag = [diag_ref[k, k * TILE : (k + 1) * TILE, :] for k in range(blocks)]
    inv = []
    for block in diag:
        on_diag = jnp.where(eye, block, 0.0)
        down = 1.0 / jnp.sum(on_diag, axis=1, keepdims=True)
        along = 1.0 / jnp.sum(on_diag, axis=0, keepdims=True)
        pair = (rows // 2 == cols // 2) & (rows > cols)
        inv.append(jnp.where(eye, down, 0.0) - jnp.where(pair, down * block * along, 0.0))
    size = 2
    while size < TILE:
        joined = (rows // (2 * size) == cols // (2 * size)) & (rows // size > cols // size)
        right = [exact_dot(jnp.where(joined, d, 0.0), i) for d, i in zip(diag, inv)]
        inv = [i - exact_dot(i, r) for i, r in zip(inv, right)]
        size *= 2
    inv_ref[...] = jnp.zeros((NB, NB), jnp.float32)
    for k in range(blocks):
        inv_ref[k * TILE : (k + 1) * TILE, k * TILE : (k + 1) * TILE] = inv[k]
    for k in (0, 2):
        lower = diag_ref[k, (k + 1) * TILE : (k + 2) * TILE, :]
        inv_ref[(k + 1) * TILE : (k + 2) * TILE, k * TILE : (k + 1) * TILE] = -exact_dot(
            inv[k + 1], exact_dot(lower, inv[k])
        )
    half = NB // 2
    corner = jnp.concatenate([diag_ref[0, half:, :], diag_ref[1, half:, :]], axis=1)
    inv_ref[half:, :half] = -exact_dot(inv_ref[half:, half:], exact_dot(corner, inv_ref[:half, :half]))


def inverse_of(diag_cols):
    return pl.pallas_call(
        inverse_kernel,
        out_shape=jax.ShapeDtypeStruct((NB, NB), jnp.float32),
        name="lower_inverse",
    )(diag_cols)


def panel_blocks(block):
    y, k = lax.axis_index("y"), lax.axis_index("k")
    near = lax.ppermute(block, "y", [(2, 1), (3, 0)])
    across = lax.ppermute(block, "y", [(2, 3), (3, 2)])
    far = lax.ppermute(block, "y", [(2, 0), (3, 1)])
    two = jnp.where(y == 2, block, jnp.where(y == 3, across, jnp.where(y == 1, near, far)))
    three = jnp.where(y == 3, block, jnp.where(y == 2, across, jnp.where(y == 0, near, far)))
    mine = jnp.stack([two, three])
    other = lax.ppermute(mine, "k", [(0, 1), (1, 0)])
    first, second = jnp.where(k == 0, mine, other), jnp.where(k == 0, other, mine)
    return jnp.stack([first[0], second[0], first[1], second[1]])


def to_all(block, axis):
    size = lax.axis_size(axis)
    return lax.all_to_all(
        jnp.broadcast_to(block[None], (size, *block.shape)), axis, 0, 0, tiled=True
    )


def side_by_side(blocks):
    return jnp.moveaxis(blocks, 0, 1).reshape(blocks.shape[1], -1)


def local(factor, adjoint):
    z, row = lax.axis_index("z"), lax.axis_index(ROW)
    col = lax.axis_index("y") * 2 + lax.axis_index("k")
    low = z >= 4
    owner = col >= 4
    f0, f1, f2 = (factor[:, :, e, :].reshape(288, TILE) for e in range(3))
    a0, a1, a2 = (adjoint[:, :, e, :].reshape(288, TILE) for e in range(3))
    own_rows = row * 32 + jnp.arange(32, dtype=jnp.int32)
    own_cols = col * TILE + jnp.arange(TILE, dtype=jnp.int32)
    a2_top = jnp.where(own_cols[None, :] > own_rows[:, None], 0.0, a2[:32])
    a2 = jnp.concatenate([a2_top, a2[32:]], 0)

    last = to_all(f2[:32], ROW)[16:].reshape(NB, TILE)
    left = jnp.concatenate([f0[:32], f1[:32]], 1)
    handed = lax.ppermute(left[16:], "z", [(i, i - 4) for i in range(4, 8)])
    sent = jnp.where(low, left[:16], handed)
    arrived = to_all(sent, ROW)
    left_rows = jnp.stack([arrived[16:], arrived[:16]], 1).reshape(NB, 2 * TILE)

    panels = panel_blocks(jnp.concatenate([a2, f2], 0))
    diag_cols = panel_blocks(last)
    inverse = inverse_of(diag_cols)

    adj_panel = side_by_side(panels[:, :288])
    fac_panel = side_by_side(panels[:, 288:])
    weights = adj_panel[32:]
    top = jnp.where(low, 1.0, 0.0)
    first = jnp.concatenate([fac_panel[:32] * top, weights], 0)
    second = jnp.concatenate([-adj_panel[:32] * top, fac_panel[32:]], 0)
    steps = jnp.arange(NB, dtype=jnp.int32)
    kept = steps[:, None] >= steps[None, :]
    over_rows = ((0,), (0,))
    middle = -jnp.where(
        kept, exact_dot(first, second, over_rows), exact_dot(second, first, over_rows)
    )
    eye_cols = (steps[:, None] == (own_cols - 512)[None, :]).astype(jnp.float32)
    right = jnp.concatenate([left_rows, jnp.where(owner, eye_cols, last)], 1)
    below = jnp.concatenate([f0[32:], f1[32:], jnp.where(owner, 0.0, f2[32:])], 1)
    solved = exact_dot(inverse, right)
    inner = exact_dot(weights, below, over_rows) + exact_dot(middle, solved)
    partial = exact_dot(inverse, inner, over_rows)
    halves = partial.reshape(16, 2, 16, 3 * TILE)
    parts = jnp.concatenate([halves[:, 1], halves[:, 0]], 0)
    share = lax.all_to_all(parts, ROW, 0, 0, tiled=True).sum(axis=0)
    partner = lax.ppermute(share, "z", [(i, i + 4) for i in range(4)])
    change = jnp.concatenate([share, partner], 0)

    update = exact_dot(weights, solved)
    tops = jnp.concatenate([a0[:32], a1[:32], a2_top], 1)
    gap = own_rows[:, None] - own_cols[None, :]
    halved = jnp.where(gap > 0, 1.0, jnp.where(gap == 0, 0.5, 0.0)) * change[:, 2 * TILE :]
    new_diag = jnp.where(owner, halved, tops[:, 2 * TILE :] - change[:, 2 * TILE :])
    new_top = jnp.concatenate([tops[:, : 2 * TILE] - change[:, : 2 * TILE], new_diag], 1)
    new_top = jnp.where(low, new_top, tops)
    new_below = jnp.concatenate(
        [
            a0[32:] - update[:, :TILE],
            a1[32:] - update[:, TILE : 2 * TILE],
            jnp.where(owner, update[:, 2 * TILE :], a2[32:] - update[:, 2 * TILE :]),
        ],
        1,
    )
    return jnp.concatenate([new_top, new_below], 0).reshape(9, 32, 3, TILE)


def solution(mesh):
    split = Mesh(mesh.devices.reshape(8, 4, 4, 2), ("z", "x", "y", "k"))
    placed = P(None, ROW, None, ("y", "k"))
    return jax.shard_map(
        local, mesh=split, in_specs=(placed, placed), out_specs=placed, check_vma=False
    )
```

```python
import jax
import jax.numpy as jnp
from jax import lax
from jax.experimental import pallas as pl
from jax.experimental.pallas import tpu as pltpu
from jax.sharding import Mesh
from jax.sharding import PartitionSpec as P

NB = 512
TILE = 128
WIDE = 3 * TILE
ROW = ("zh", "zl", "x")


def exact_dot(first, second, over=((1,), (0,)), precision=lax.Precision.HIGHEST):
    return lax.dot_general(
        first, second, (over, ((), ())),
        precision=precision, preferred_element_type=jnp.float32,
    )


def close_dot(first, second, over=((1,), (0,))):
    return exact_dot(first, second, over, lax.Precision.HIGH)


def split(value):
    high = value.astype(jnp.bfloat16)
    return high, (value - high.astype(jnp.float32)).astype(jnp.bfloat16)


def split_dot(first, second, over=((1,), (0,))):
    def dot(a, b):
        return lax.dot_general(a, b, (over, ((), ())), preferred_element_type=jnp.float32)

    return dot(first[0], second[0]) + (dot(first[0], second[1]) + dot(first[1], second[0]))


def blocks_inverse(diag_ref, inv_ref):
    rows = lax.broadcasted_iota(jnp.int32, (TILE, TILE), 0)
    cols = lax.broadcasted_iota(jnp.int32, (TILE, TILE), 1)
    blocks = NB // TILE
    eye = rows == cols
    diag = [diag_ref[k, k * TILE : (k + 1) * TILE, :] for k in range(blocks)]
    inv = []
    for block in diag:
        on_diag = jnp.where(eye, block, 0.0)
        down = 1.0 / jnp.sum(on_diag, axis=1, keepdims=True)
        along = 1.0 / jnp.sum(on_diag, axis=0, keepdims=True)
        pair = (rows // 2 == cols // 2) & (rows > cols)
        inv.append(jnp.where(eye, down, 0.0) - jnp.where(pair, down * block * along, 0.0))
    size = 2
    while size < TILE:
        joined = (rows // (2 * size) == cols // (2 * size)) & (rows // size > cols // size)
        right = [exact_dot(jnp.where(joined, d, 0.0), i) for d, i in zip(diag, inv)]
        inv = [i - exact_dot(i, r) for i, r in zip(inv, right)]
        size *= 2
    inv_ref[...] = jnp.zeros((NB, NB), jnp.float32)
    for k in range(blocks):
        inv_ref[k * TILE : (k + 1) * TILE, k * TILE : (k + 1) * TILE] = inv[k]
    for k in (0, 2):
        lower = diag_ref[k, (k + 1) * TILE : (k + 2) * TILE, :]
        inv_ref[(k + 1) * TILE : (k + 2) * TILE, k * TILE : (k + 1) * TILE] = -exact_dot(
            inv[k + 1], exact_dot(lower, inv[k])
        )
    half = NB // 2
    corner = jnp.concatenate([diag_ref[0, half:, :], diag_ref[1, half:, :]], axis=1)
    inv_ref[half:, :half] = -exact_dot(inv_ref[half:, half:], exact_dot(corner, inv_ref[:half, :half]))


def solve_kernel(
    place, pack0, pack1, pack2, pack3, left0, left1, left2, left3, outer, middle,
    solved_ref, part0, part1, part2, part3, diag, inv, right, partial,
):
    x, owner, offset = (place[i] for i in range(3))
    rows = lax.broadcasted_iota(jnp.int32, (32, TILE), 0)
    cols = lax.broadcasted_iota(jnp.int32, (32, TILE), 1) + offset
    packs, lefts = (pack0, pack1, pack2, pack3), (left0, left1, left2, left3)
    for step in range(4):
        at = 0
        for block in range(4):
            for zl in range(block, 4):
                start = pl.multiple_of((zl * 4 + (x - step) % 4) * 32, 32)
                diag[block, pl.ds(start, 32), :] = packs[step][at : at + 32, :]
                at += 32
        for zl in range(4):
            start = pl.multiple_of((zl * 4 + (x - step) % 4) * 32, 32)
            line = lefts[step][zl * 32 : (zl + 1) * 32, :]
            eye = (rows + start == cols).astype(jnp.float32)
            right[pl.ds(start, 32), : 2 * TILE] = line[:, : 2 * TILE]
            right[pl.ds(start, 32), 2 * TILE :] = jnp.where(owner == 1, eye, line[:, 2 * TILE :])
    blocks_inverse(diag, inv)
    inverse = split(inv[...])
    solved = split_dot(inverse, split(right[...]))
    solved_ref[...] = solved
    inner = outer[...] + split_dot(split(middle[...]), split(solved))
    partial[...] = split_dot(inverse, split(inner), ((0,), (0,)))
    for step, part in enumerate((part0, part1, part2, part3)):
        for zl in range(4):
            start = pl.multiple_of((zl * 4 + (x + step) % 4) * 32, 32)
            part[zl * 32 : (zl + 1) * 32, :] = partial[pl.ds(start, 32), :]


def spread_kernel(part0, part1, part2, part3, out):
    total = (part0[...] + part1[...]) + (part2[...] + part3[...])
    for zl in range(4):
        out[zl] = jnp.zeros((32, WIDE), jnp.float32)
        out[4 + zl] = total[zl * 32 : (zl + 1) * 32, :]


def spread_sum(*parts):
    parts = [pltpu.with_memory_space_constraint(p, pltpu.VMEM) for p in parts]
    return pl.pallas_call(
        spread_kernel,
        out_shape=pltpu.VMEM((8, 32, WIDE), jnp.float32),
        in_specs=[pl.BlockSpec(memory_space=pltpu.VMEM)] * 4,
        out_specs=pl.BlockSpec(memory_space=pltpu.VMEM),
        compiler_params=pltpu.CompilerParams(vmem_limit_bytes=8 << 20),
        name="spread",
    )(*parts)


def solved_parts(place, *arrays):
    arrays = [pltpu.with_memory_space_constraint(a, pltpu.VMEM) for a in arrays]
    part = pltpu.VMEM((TILE, WIDE), jnp.float32)
    return pl.pallas_call(
        solve_kernel,
        out_shape=(pltpu.VMEM((NB, WIDE), jnp.float32),) + (part,) * 4,
        in_specs=[pl.BlockSpec(memory_space=pltpu.SMEM)]
        + [pl.BlockSpec(memory_space=pltpu.VMEM)] * len(arrays),
        out_specs=(pl.BlockSpec(memory_space=pltpu.VMEM),) * 5,
        scratch_shapes=[
            pltpu.VMEM((4, NB, TILE), jnp.float32),
            pltpu.VMEM((NB, NB), jnp.float32),
            pltpu.VMEM((NB, WIDE), jnp.float32),
            pltpu.VMEM((NB, WIDE), jnp.float32),
        ],
        compiler_params=pltpu.CompilerParams(vmem_limit_bytes=24 << 20),
        name="solve",
    )(place, *arrays)


def over_x(block):
    blocks = block if isinstance(block, tuple) else (block,) * 3
    return tuple(
        lax.ppermute(b, "x", [(i, (i + s) % 4) for i in range(4)])
        for s, b in zip((1, 2, 3), blocks)
    )


def over_y(block):
    near = lax.ppermute(block, "y", [(2, 1), (3, 0)])
    across = lax.ppermute(block, "y", [(2, 3), (3, 2)])
    far = lax.ppermute(block, "y", [(2, 0), (3, 1)])
    return near, across, far


def own_pair(block, near, across, far):
    inside = lax.axis_index("y") >= 2
    return jnp.where(inside, across, near), jnp.where(inside, block, far)


def swap(value):
    return lax.ppermute(value, "k", [(0, 1), (1, 0)])


def ordered(near, rest, other_near, other_rest):
    odd, k = lax.axis_index("y") % 2 == 1, lax.axis_index("k") == 1
    low, high = jnp.where(odd, near, rest), jnp.where(odd, rest, near)
    other_low = jnp.where(odd, other_near, other_rest)
    other_high = jnp.where(odd, other_rest, other_near)
    return (
        jnp.where(k, other_low, low), jnp.where(k, low, other_low),
        jnp.where(k, other_high, high), jnp.where(k, high, other_high),
    )


def panel_blocks(block, sent, earlier):
    sent = lax.optimization_barrier((*sent, earlier))[:3]
    near, rest = own_pair(block, *sent)
    return ordered(near, rest, swap(near), swap(rest))


def to_all(block, axis):
    size = lax.axis_size(axis)
    return lax.all_to_all(
        jnp.broadcast_to(block[None], (size, *block.shape)), axis, 0, 0, tiled=True
    )


def step(factor, adjoint):
    row, x = lax.axis_index(ROW), lax.axis_index("x")
    col = lax.axis_index("y") * 2 + lax.axis_index("k")
    low = lax.axis_index("zh") == 1
    owner = col >= 4
    f0, f1, f2 = (factor[:, :, e, :].reshape(288, TILE) for e in range(3))
    a0, a1, a2 = (adjoint[:, :, e, :].reshape(288, TILE) for e in range(3))
    own_rows = row * 32 + jnp.arange(32, dtype=jnp.int32)
    own_cols = col * TILE + jnp.arange(TILE, dtype=jnp.int32)
    a2_top = jnp.where(own_cols[None, :] > own_rows[:, None], 0.0, a2[:32])
    a2 = jnp.concatenate([a2_top, a2[32:]], 0)

    tops_l = jnp.concatenate([f0[:32], f1[:32], f2[:32]], 1)
    lines = to_all(tops_l, ("zh", "zl"))[4:].reshape(TILE, WIDE)
    sent = over_y(jnp.concatenate([a2, f2], 0))
    last = lines[:, 2 * TILE :]
    near, rest = own_pair(last, *over_y(last))
    lefts = (lines, *over_x(lines))
    quads = ordered(near, rest, swap(near), swap(rest))
    pack = jnp.concatenate([quads[c][32 * c :] for c in range(4)], 0)
    packs = (pack, *over_x(pack))
    panels = panel_blocks(jnp.concatenate([a2, f2], 0), sent, near)
    adj_panel = jnp.concatenate([p[:288] for p in panels], 1)
    fac_panel = jnp.concatenate([p[288:] for p in panels], 1)

    weights = adj_panel[32:]
    top = jnp.where(low, 1.0, 0.0)
    first = jnp.concatenate([fac_panel[:32] * top, weights], 0)
    second = jnp.concatenate([-adj_panel[:32] * top, fac_panel[32:]], 0)
    steps = jnp.arange(NB, dtype=jnp.int32)
    kept = steps[:, None] >= steps[None, :]
    over_rows = ((0,), (0,))
    middle = -jnp.where(
        kept, close_dot(first, second, over_rows), close_dot(second, first, over_rows)
    )
    below = jnp.concatenate([f0[32:], f1[32:], jnp.where(owner, 0.0, f2[32:])], 1)
    outer = close_dot(weights, below, over_rows)
    place = jnp.stack(
        [x, owner.astype(jnp.int32), col * TILE - 512]
    ).astype(jnp.int32)
    solved, *parts = solved_parts(place, *packs, *lefts, outer, middle)
    moved = over_x(tuple(parts[1:]))
    spread = spread_sum(parts[0], *moved)
    change = lax.all_to_all(spread, ("zh", "zl"), 0, 0, tiled=True).sum(axis=0)

    update = close_dot(weights, solved)
    tops = jnp.concatenate([a0[:32], a1[:32], a2_top], 1)
    gap = own_rows[:, None] - own_cols[None, :]
    halved = jnp.where(gap > 0, 1.0, jnp.where(gap == 0, 0.5, 0.0)) * change[:, 2 * TILE :]
    new_diag = jnp.where(owner, halved, tops[:, 2 * TILE :] - change[:, 2 * TILE :])
    new_top = jnp.concatenate([tops[:, : 2 * TILE] - change[:, : 2 * TILE], new_diag], 1)
    new_top = jnp.where(low, new_top, tops)
    new_below = jnp.concatenate(
        [
            a0[32:] - update[:, :TILE],
            a1[32:] - update[:, TILE : 2 * TILE],
            jnp.where(owner, update[:, 2 * TILE :], a2[32:] - update[:, 2 * TILE :]),
        ],
        1,
    )
    return jnp.concatenate([new_top, new_below], 0).reshape(9, 32, 3, TILE)


def solution(mesh):
    split_mesh = Mesh(
        mesh.devices.reshape(2, 4, 4, 4, 2), ("zh", "zl", "x", "y", "k")
    )
    placed = P(None, ROW, None, ("y", "k"))
    return jax.shard_map(
        step, mesh=split_mesh, in_specs=(placed, placed), out_specs=placed, check_vma=False
    )
```

```python
import jax
import jax.numpy as jnp
from jax import lax
from jax.experimental import pallas as pl
from jax.experimental.pallas import tpu as pltpu
from jax.sharding import Mesh
from jax.sharding import PartitionSpec as P

NB = 512
TILE = 128
WIDE = 3 * TILE
ROW = ("zh", "zl", "x")


def exact_dot(first, second, over=((1,), (0,)), precision=lax.Precision.HIGHEST):
    return lax.dot_general(
        first, second, (over, ((), ())),
        precision=precision, preferred_element_type=jnp.float32,
    )


def close_dot(first, second, over=((1,), (0,))):
    return exact_dot(first, second, over, lax.Precision.HIGH)


def split(value):
    high = value.astype(jnp.bfloat16)
    return high, (value - high.astype(jnp.float32)).astype(jnp.bfloat16)


def split_dot(first, second, over=((1,), (0,))):
    def dot(a, b):
        return lax.dot_general(a, b, (over, ((), ())), preferred_element_type=jnp.float32)

    return dot(first[0], second[0]) + (dot(first[0], second[1]) + dot(first[1], second[0]))


def brief_dot(first, second):
    (a, b), (c, d) = split(first), split(second)
    return jnp.dot(
        jnp.concatenate([a, a, b], 1),
        jnp.concatenate([c, d, c], 0),
        preferred_element_type=jnp.float32,
    )


def blocks_inverse(diag_ref, inv_ref):
    rows = lax.broadcasted_iota(jnp.int32, (TILE, TILE), 0)
    cols = lax.broadcasted_iota(jnp.int32, (TILE, TILE), 1)
    blocks = NB // TILE
    eye = rows == cols
    diag = [diag_ref[k, k * TILE : (k + 1) * TILE, :] for k in range(blocks)]
    inv = []
    for block in diag:
        on_diag = jnp.where(eye, block, 0.0)
        down = 1.0 / jnp.sum(on_diag, axis=1, keepdims=True)
        along = 1.0 / jnp.sum(on_diag, axis=0, keepdims=True)
        pair = (rows // 2 == cols // 2) & (rows > cols)
        inv.append(jnp.where(eye, down, 0.0) - jnp.where(pair, down * block * along, 0.0))
    size = 2
    while size < TILE:
        joined = (rows // (2 * size) == cols // (2 * size)) & (rows // size > cols // size)
        right = [brief_dot(jnp.where(joined, d, 0.0), i) for d, i in zip(diag, inv)]
        inv = [i - brief_dot(i, r) for i, r in zip(inv, right)]
        size *= 2
    inv_ref[...] = jnp.zeros((NB, NB), jnp.float32)
    for k in range(blocks):
        inv_ref[k * TILE : (k + 1) * TILE, k * TILE : (k + 1) * TILE] = inv[k]
    for k in (0, 2):
        lower = diag_ref[k, (k + 1) * TILE : (k + 2) * TILE, :]
        inv_ref[(k + 1) * TILE : (k + 2) * TILE, k * TILE : (k + 1) * TILE] = -brief_dot(
            inv[k + 1], brief_dot(lower, inv[k])
        )
    half = NB // 2
    corner = jnp.concatenate([diag_ref[0, half:, :], diag_ref[1, half:, :]], axis=1)
    inv_ref[half:, :half] = -brief_dot(inv_ref[half:, half:], brief_dot(corner, inv_ref[:half, :half]))


def solve_kernel(
    place, pack0, pack1, pack2, pack3, left0, left1, left2, left3, outer, middle,
    solved_ref, part0, part1, part2, part3, diag, inv, right, partial,
):
    x, owner, offset = (place[i] for i in range(3))
    rows = lax.broadcasted_iota(jnp.int32, (32, TILE), 0)
    cols = lax.broadcasted_iota(jnp.int32, (32, TILE), 1) + offset
    packs, lefts = (pack0, pack1, pack2, pack3), (left0, left1, left2, left3)
    for step in range(4):
        at = 0
        for block in range(4):
            for zl in range(block, 4):
                start = pl.multiple_of((zl * 4 + (x - step) % 4) * 32, 32)
                diag[block, pl.ds(start, 32), :] = packs[step][at : at + 32, :]
                at += 32
        for zl in range(4):
            start = pl.multiple_of((zl * 4 + (x - step) % 4) * 32, 32)
            eye = (rows + start == cols).astype(jnp.float32)
            right[pl.ds(start, 32), :TILE] = lefts[step][zl, 0]
            right[pl.ds(start, 32), TILE : 2 * TILE] = lefts[step][zl, 1]
            right[pl.ds(start, 32), 2 * TILE :] = jnp.where(owner == 1, eye, lefts[step][zl, 2])
    blocks_inverse(diag, inv)
    inverse = split(inv[...])
    solved = split_dot(inverse, split(right[...]))
    solved_ref[...] = solved
    inner = outer[...] + split_dot(split(middle[...]), split(solved))
    partial[...] = split_dot(inverse, split(inner), ((0,), (0,)))
    for step, part in enumerate((part0, part1, part2, part3)):
        for zl in range(4):
            start = pl.multiple_of((zl * 4 + (x + step) % 4) * 32, 32)
            for e in range(3):
                part[zl, e] = partial[pl.ds(start, 32), e * TILE : (e + 1) * TILE]


def spread_kernel(part0, part1, part2, part3, out):
    for zl in range(4):
        total = (part0[zl] + part1[zl]) + (part2[zl] + part3[zl])
        out[(zl + 2) % 4] = total[:, :16]
        out[4 + zl] = total[:, 16:]


def spread_sum(*parts):
    parts = [pltpu.with_memory_space_constraint(p, pltpu.VMEM) for p in parts]
    return pl.pallas_call(
        spread_kernel,
        out_shape=pltpu.VMEM((8, 3, 16, TILE), jnp.float32),
        in_specs=[pl.BlockSpec(memory_space=pltpu.VMEM)] * 4,
        out_specs=pl.BlockSpec(memory_space=pltpu.VMEM),
        compiler_params=pltpu.CompilerParams(vmem_limit_bytes=8 << 20),
        name="spread",
    )(*parts)


def finish_kernel(place, base, tops, share, other, out, stage, sem):
    low, owner, gap = place[0], place[1], place[2]

    @pl.when(low == 1)
    def _():
        change = jnp.concatenate([other[...], share[...]], axis=1)
        away = (
            lax.broadcasted_iota(jnp.int32, (32, TILE), 0)
            - lax.broadcasted_iota(jnp.int32, (32, TILE), 1)
            + gap
        )
        halved = jnp.where(away > 0, 1.0, jnp.where(away == 0, 0.5, 0.0)) * change[2]
        stage[0] = tops[0] - change[0]
        stage[1] = tops[1] - change[1]
        stage[2] = jnp.where(owner == 1, halved, tops[2] - change[2])
        copy = pltpu.make_async_copy(stage, out.at[0], sem)
        copy.start()
        copy.wait()


def finished(place, base, tops, share, other):
    small = [pltpu.with_memory_space_constraint(a, pltpu.VMEM) for a in (tops, share, other)]
    return pl.pallas_call(
        finish_kernel,
        out_shape=jax.ShapeDtypeStruct(base.shape, jnp.float32),
        in_specs=[pl.BlockSpec(memory_space=pltpu.SMEM), pl.BlockSpec(memory_space=pl.ANY)]
        + [pl.BlockSpec(memory_space=pltpu.VMEM)] * 3,
        out_specs=pl.BlockSpec(memory_space=pl.ANY),
        scratch_shapes=[pltpu.VMEM((3, 32, TILE), jnp.float32), pltpu.SemaphoreType.DMA],
        input_output_aliases={1: 0},
        compiler_params=pltpu.CompilerParams(vmem_limit_bytes=4 << 20),
        name="finish",
    )(place, base, *small)


def solved_parts(place, *arrays):
    arrays = [pltpu.with_memory_space_constraint(a, pltpu.VMEM) for a in arrays]
    part = pltpu.VMEM((4, 3, 32, TILE), jnp.float32)
    return pl.pallas_call(
        solve_kernel,
        out_shape=(pltpu.VMEM((NB, WIDE), jnp.float32),) + (part,) * 4,
        in_specs=[pl.BlockSpec(memory_space=pltpu.SMEM)]
        + [pl.BlockSpec(memory_space=pltpu.VMEM)] * len(arrays),
        out_specs=(pl.BlockSpec(memory_space=pltpu.VMEM),) * 5,
        scratch_shapes=[
            pltpu.VMEM((4, NB, TILE), jnp.float32),
            pltpu.VMEM((NB, NB), jnp.float32),
            pltpu.VMEM((NB, WIDE), jnp.float32),
            pltpu.VMEM((NB, WIDE), jnp.float32),
        ],
        compiler_params=pltpu.CompilerParams(vmem_limit_bytes=24 << 20),
        name="solve",
    )(place, *arrays)


def copies_kernel(source, out):
    for z in range(8):
        out[z] = source[0]


def copies(source):
    block = source.shape[1:]
    return pl.pallas_call(
        copies_kernel,
        grid=(1,),
        out_shape=pltpu.VMEM((8, *block), jnp.float32),
        in_specs=[pl.BlockSpec((1, *block), lambda i: (0, 0, 0, 0))],
        out_specs=pl.BlockSpec(memory_space=pltpu.VMEM),
        compiler_params=pltpu.CompilerParams(vmem_limit_bytes=4 << 20),
        name="copies",
    )(pltpu.with_memory_space_constraint(source, pltpu.HBM))


def over_x(block):
    blocks = block if isinstance(block, tuple) else (block,) * 3
    return tuple(
        lax.ppermute(b, "x", [(i, (i + s) % 4) for i in range(4)])
        for s, b in zip((1, 2, 3), blocks)
    )


def over_y(block):
    near = lax.ppermute(block, "y", [(2, 1), (3, 0)])
    across = lax.ppermute(block, "y", [(2, 3), (3, 2)])
    far = lax.ppermute(block, "y", [(2, 0), (3, 1)])
    return near, across, far


def own_pair(block, near, across, far):
    inside = lax.axis_index("y") >= 2
    return jnp.where(inside, across, near), jnp.where(inside, block, far)


def swap(value):
    return lax.ppermute(value, "k", [(0, 1), (1, 0)])


def ordered(near, rest, other_near, other_rest):
    odd, k = lax.axis_index("y") % 2 == 1, lax.axis_index("k") == 1
    low, high = jnp.where(odd, near, rest), jnp.where(odd, rest, near)
    other_low = jnp.where(odd, other_near, other_rest)
    other_high = jnp.where(odd, other_rest, other_near)
    return (
        jnp.where(k, other_low, low), jnp.where(k, low, other_low),
        jnp.where(k, other_high, high), jnp.where(k, high, other_high),
    )


def panel_blocks(block, sent, earlier):
    sent = lax.optimization_barrier((*sent, earlier))[:3]
    near, rest = own_pair(block, *sent)
    return ordered(near, rest, swap(near), swap(rest))


def step(factor, adjoint):
    row, x = lax.axis_index(ROW), lax.axis_index("x")
    col = lax.axis_index("y") * 2 + lax.axis_index("k")
    low = lax.axis_index("zh") == 1
    owner = col >= 4
    factor, adjoint = factor.transpose(0, 2, 1, 3), adjoint.transpose(0, 2, 1, 3)
    f2, a2 = factor[:, 2].reshape(288, TILE), adjoint[:, 2].reshape(288, TILE)
    own_rows = row * 32 + jnp.arange(32, dtype=jnp.int32)
    own_cols = col * TILE + jnp.arange(TILE, dtype=jnp.int32)
    a2_top = jnp.where(own_cols[None, :] > own_rows[:, None], 0.0, a2[:32])
    a2 = jnp.concatenate([a2_top, a2[32:]], 0)

    lines = lax.all_to_all(copies(factor), ("zh", "zl"), 0, 0, tiled=True)[4:]
    both = jnp.concatenate([a2, f2], 0)
    near = lax.ppermute(both, "y", [(2, 1), (3, 0)])
    across = lax.ppermute(both, "y", [(2, 3), (3, 2)])
    sent = near, across, lax.ppermute(both, "y", [(2, 0), (3, 1)])
    last = lines[:, 2].reshape(TILE, TILE)
    low_block, rest = own_pair(last, *over_y(last))
    lefts = (lines, *over_x(lines))
    quads = ordered(low_block, rest, swap(low_block), swap(rest))
    pack = jnp.concatenate([quads[c][32 * c :] for c in range(4)], 0)
    packs = (pack, *over_x(pack))
    panels = panel_blocks(both, sent, low_block)
    adj_panel = jnp.concatenate([p[:288] for p in panels], 1)
    fac_panel = jnp.concatenate([p[288:] for p in panels], 1)

    weights = adj_panel[32:]
    top = jnp.where(low, 1.0, 0.0)
    first = jnp.concatenate([fac_panel[:32] * top, weights], 0)
    second = jnp.concatenate([-adj_panel[:32] * top, fac_panel[32:]], 0)
    steps = jnp.arange(NB, dtype=jnp.int32)
    kept = steps[:, None] >= steps[None, :]
    over_rows = ((0,), (0,))
    middle = -jnp.where(
        kept, close_dot(first, second, over_rows), close_dot(second, first, over_rows)
    )
    f0, f1 = (factor[1:, e].reshape(256, TILE) for e in range(2))
    below = jnp.concatenate([f0, f1, jnp.where(owner, 0.0, f2[32:])], 1)
    outer = close_dot(weights, below, over_rows)
    place = jnp.stack(
        [x, owner.astype(jnp.int32), col * TILE - 512]
    ).astype(jnp.int32)
    solved, *parts = solved_parts(place, *packs, *lefts, outer, middle)
    moved = over_x(tuple(parts[1:]))
    spread = spread_sum(parts[0], *moved)
    share = lax.all_to_all(spread, ("zh", "zl"), 0, 0, tiled=True).sum(axis=0)
    other = lax.ppermute(share, ("zh", "zl"), [(i, 4 + (i + 2) % 4) for i in range(4)])

    update = close_dot(weights, solved).reshape(8, 32, 3, TILE).transpose(0, 2, 1, 3)
    tops = jnp.concatenate([adjoint[0, :2], a2_top[None]], 0)
    new_col = jnp.where(owner, update[:, 2], adjoint[1:, 2] - update[:, 2])
    below = jnp.concatenate([adjoint[1:, :2] - update[:, :2], new_col[:, None]], 1)
    base = jnp.concatenate([tops[None], below], 0)
    end_place = jnp.stack(
        [low.astype(jnp.int32), owner.astype(jnp.int32), row * 32 - col * TILE]
    ).astype(jnp.int32)
    return finished(end_place, base, tops, share, other).transpose(0, 2, 1, 3)


def solution(mesh):
    split_mesh = Mesh(
        mesh.devices.reshape(2, 4, 4, 4, 2), ("zh", "zl", "x", "y", "k")
    )
    placed = P(None, ROW, None, ("y", "k"))
    return jax.shard_map(
        step, mesh=split_mesh, in_specs=(placed, placed), out_specs=placed, check_vma=False
    )
```

```python
import jax
import jax.numpy as jnp
from jax import lax
from jax.experimental import pallas as pl
from jax.experimental.pallas import tpu as pltpu
from jax.sharding import Mesh
from jax.sharding import PartitionSpec as P

NB = 512
TILE = 128
WIDE = 3 * TILE
ROW = ("zh", "zl", "x")


def exact_dot(first, second, over=((1,), (0,)), precision=lax.Precision.HIGHEST):
    return lax.dot_general(
        first, second, (over, ((), ())),
        precision=precision, preferred_element_type=jnp.float32,
    )


def close_dot(first, second, over=((1,), (0,))):
    return exact_dot(first, second, over, lax.Precision.HIGH)


def split(value):
    high = value.astype(jnp.bfloat16)
    return high, (value - high.astype(jnp.float32)).astype(jnp.bfloat16)


def split_dot(first, second, over=((1,), (0,))):
    def dot(a, b):
        return lax.dot_general(a, b, (over, ((), ())), preferred_element_type=jnp.float32)

    return dot(first[0], second[0]) + (dot(first[0], second[1]) + dot(first[1], second[0]))


def brief_dot(first, second):
    (a, b), (c, d) = split(first), split(second)
    return jnp.dot(
        jnp.concatenate([a, a, b], 1),
        jnp.concatenate([c, d, c], 0),
        preferred_element_type=jnp.float32,
    )


def blocks_inverse(diag_ref, inv_ref):
    rows = lax.broadcasted_iota(jnp.int32, (TILE, TILE), 0)
    cols = lax.broadcasted_iota(jnp.int32, (TILE, TILE), 1)
    blocks = NB // TILE
    eye = rows == cols
    diag = [diag_ref[k, k * TILE : (k + 1) * TILE, :] for k in range(blocks)]
    inv = []
    for block in diag:
        on_diag = jnp.where(eye, block, 0.0)
        down = 1.0 / jnp.sum(on_diag, axis=1, keepdims=True)
        along = 1.0 / jnp.sum(on_diag, axis=0, keepdims=True)
        pair = (rows // 2 == cols // 2) & (rows > cols)
        inv.append(jnp.where(eye, down, 0.0) - jnp.where(pair, down * block * along, 0.0))
    size = 2
    while size < TILE:
        joined = (rows // (2 * size) == cols // (2 * size)) & (rows // size > cols // size)
        right = [brief_dot(jnp.where(joined, d, 0.0), i) for d, i in zip(diag, inv)]
        inv = [i - brief_dot(i, r) for i, r in zip(inv, right)]
        size *= 2
    inv_ref[...] = jnp.zeros((NB, NB), jnp.float32)
    for k in range(blocks):
        inv_ref[k * TILE : (k + 1) * TILE, k * TILE : (k + 1) * TILE] = inv[k]
    for k in (0, 2):
        lower = diag_ref[k, (k + 1) * TILE : (k + 2) * TILE, :]
        inv_ref[(k + 1) * TILE : (k + 2) * TILE, k * TILE : (k + 1) * TILE] = -brief_dot(
            inv[k + 1], brief_dot(lower, inv[k])
        )
    half = NB // 2
    corner = jnp.concatenate([diag_ref[0, half:, :], diag_ref[1, half:, :]], axis=1)
    inv_ref[half:, :half] = -brief_dot(inv_ref[half:, half:], brief_dot(corner, inv_ref[:half, :half]))


def solve_kernel(
    place, pack0, pack1, pack2, pack3, twin0, twin1, twin2, twin3,
    left0, left1, left2, left3, outer, middle,
    solved_ref, part0, part1, part2, part3, diag, inv, right, partial,
):
    x, owner, offset, second = (place[i] for i in range(4))
    rows = lax.broadcasted_iota(jnp.int32, (32, TILE), 0)
    cols = lax.broadcasted_iota(jnp.int32, (32, TILE), 1) + offset
    packs, twins = (pack0, pack1, pack2, pack3), (twin0, twin1, twin2, twin3)
    lefts = (left0, left1, left2, left3)
    for step in range(4):
        for at in range(6):
            zl, block = (at, 0) if at < 4 else (at - 2, 2)
            to = pl.ds(pl.multiple_of((zl * 4 + (x - step) % 4) * 32, 32), 32)
            mine = packs[step][at * 32 : (at + 1) * 32, :]
            other = twins[step][at * 32 : (at + 1) * 32, :]
            diag[block, to, :] = jnp.where(second == 1, other, mine)
            diag[block + 1, to, :] = jnp.where(second == 1, mine, other)
        for zl in range(4):
            start = pl.multiple_of((zl * 4 + (x - step) % 4) * 32, 32)
            eye = (rows + start == cols).astype(jnp.float32)
            right[pl.ds(start, 32), :TILE] = lefts[step][zl, 0]
            right[pl.ds(start, 32), TILE : 2 * TILE] = lefts[step][zl, 1]
            right[pl.ds(start, 32), 2 * TILE :] = jnp.where(owner == 1, eye, lefts[step][zl, 2])
    blocks_inverse(diag, inv)
    inverse = split(inv[...])
    solved = split_dot(inverse, split(right[...]))
    solved_ref[...] = solved
    inner = outer[...] + split_dot(split(middle[...]), split(solved))
    partial[...] = split_dot(inverse, split(inner), ((0,), (0,)))
    for step, part in enumerate((part0, part1, part2, part3)):
        for zl in range(4):
            start = pl.multiple_of((zl * 4 + (x + step) % 4) * 32, 32)
            for e in range(3):
                part[zl, e] = partial[pl.ds(start, 32), e * TILE : (e + 1) * TILE]


def spread_kernel(part0, part1, part2, part3, out):
    for zl in range(4):
        total = (part0[zl] + part1[zl]) + (part2[zl] + part3[zl])
        out[(zl + 2) % 4] = total[:, :16]
        out[4 + zl] = total[:, 16:]


def spread_sum(*parts):
    parts = [pltpu.with_memory_space_constraint(p, pltpu.VMEM) for p in parts]
    return pl.pallas_call(
        spread_kernel,
        out_shape=pltpu.VMEM((8, 3, 16, TILE), jnp.float32),
        in_specs=[pl.BlockSpec(memory_space=pltpu.VMEM)] * 4,
        out_specs=pl.BlockSpec(memory_space=pltpu.VMEM),
        compiler_params=pltpu.CompilerParams(vmem_limit_bytes=8 << 20),
        name="spread",
    )(*parts)


def finish_kernel(place, base, tops, share, other, out, stage, sem):
    low, owner, gap = place[0], place[1], place[2]

    @pl.when(low == 1)
    def _():
        change = jnp.concatenate([other[...], share[...]], axis=1)
        away = (
            lax.broadcasted_iota(jnp.int32, (32, TILE), 0)
            - lax.broadcasted_iota(jnp.int32, (32, TILE), 1)
            + gap
        )
        halved = jnp.where(away > 0, 1.0, jnp.where(away == 0, 0.5, 0.0)) * change[2]
        stage[0] = tops[0] - change[0]
        stage[1] = tops[1] - change[1]
        stage[2] = jnp.where(owner == 1, halved, tops[2] - change[2])
        copy = pltpu.make_async_copy(stage, out.at[0], sem)
        copy.start()
        copy.wait()


def finished(place, base, tops, share, other):
    small = [pltpu.with_memory_space_constraint(a, pltpu.VMEM) for a in (tops, share, other)]
    return pl.pallas_call(
        finish_kernel,
        out_shape=jax.ShapeDtypeStruct(base.shape, jnp.float32),
        in_specs=[pl.BlockSpec(memory_space=pltpu.SMEM), pl.BlockSpec(memory_space=pl.ANY)]
        + [pl.BlockSpec(memory_space=pltpu.VMEM)] * 3,
        out_specs=pl.BlockSpec(memory_space=pl.ANY),
        scratch_shapes=[pltpu.VMEM((3, 32, TILE), jnp.float32), pltpu.SemaphoreType.DMA],
        input_output_aliases={1: 0},
        compiler_params=pltpu.CompilerParams(vmem_limit_bytes=4 << 20),
        name="finish",
    )(place, base, *small)


def solved_parts(place, *arrays):
    arrays = [pltpu.with_memory_space_constraint(a, pltpu.VMEM) for a in arrays]
    part = pltpu.VMEM((4, 3, 32, TILE), jnp.float32)
    return pl.pallas_call(
        solve_kernel,
        out_shape=(pltpu.VMEM((NB, WIDE), jnp.float32),) + (part,) * 4,
        in_specs=[pl.BlockSpec(memory_space=pltpu.SMEM)]
        + [pl.BlockSpec(memory_space=pltpu.VMEM)] * len(arrays),
        out_specs=(pl.BlockSpec(memory_space=pltpu.VMEM),) * 5,
        scratch_shapes=[
            pltpu.VMEM((4, NB, TILE), jnp.float32),
            pltpu.VMEM((NB, NB), jnp.float32),
            pltpu.VMEM((NB, WIDE), jnp.float32),
            pltpu.VMEM((NB, WIDE), jnp.float32),
        ],
        compiler_params=pltpu.CompilerParams(vmem_limit_bytes=24 << 20),
        name="solve",
    )(place, *arrays)


def copies_kernel(source, out):
    for z in range(8):
        out[z] = source[0]


def copies(source):
    block = source.shape[1:]
    return pl.pallas_call(
        copies_kernel,
        grid=(1,),
        out_shape=pltpu.VMEM((8, *block), jnp.float32),
        in_specs=[pl.BlockSpec((1, *block), lambda i: (0, 0, 0, 0))],
        out_specs=pl.BlockSpec(memory_space=pltpu.VMEM),
        compiler_params=pltpu.CompilerParams(vmem_limit_bytes=4 << 20),
        name="copies",
    )(pltpu.with_memory_space_constraint(source, pltpu.HBM))


def over_x(block):
    blocks = block if isinstance(block, tuple) else (block,) * 3
    return tuple(
        lax.ppermute(b, "x", [(i, (i + s) % 4) for i in range(4)])
        for s, b in zip((1, 2, 3), blocks)
    )


def over_y(block):
    near = lax.ppermute(block, "y", [(2, 1), (3, 0)])
    across = lax.ppermute(block, "y", [(2, 3), (3, 2)])
    far = lax.ppermute(block, "y", [(2, 0), (3, 1)])
    return near, across, far


def own_pair(block, near, across, far):
    inside = lax.axis_index("y") >= 2
    return jnp.where(inside, across, near), jnp.where(inside, block, far)


def swap(value):
    return lax.ppermute(value, "k", [(0, 1), (1, 0)])


def ordered(near, rest, other_near, other_rest):
    odd, k = lax.axis_index("y") % 2 == 1, lax.axis_index("k") == 1
    low, high = jnp.where(odd, near, rest), jnp.where(odd, rest, near)
    other_low = jnp.where(odd, other_near, other_rest)
    other_high = jnp.where(odd, other_rest, other_near)
    return (
        jnp.where(k, other_low, low), jnp.where(k, low, other_low),
        jnp.where(k, other_high, high), jnp.where(k, high, other_high),
    )


def panel_blocks(block, sent, earlier):
    sent = lax.optimization_barrier((*sent, earlier))[:3]
    near, rest = own_pair(block, *sent)
    return ordered(near, rest, swap(near), swap(rest))


def step(factor, adjoint):
    row, x = lax.axis_index(ROW), lax.axis_index("x")
    col = lax.axis_index("y") * 2 + lax.axis_index("k")
    low = lax.axis_index("zh") == 1
    owner = col >= 4
    factor, adjoint = factor.transpose(0, 2, 1, 3), adjoint.transpose(0, 2, 1, 3)
    f2, a2 = factor[:, 2].reshape(288, TILE), adjoint[:, 2].reshape(288, TILE)
    own_rows = row * 32 + jnp.arange(32, dtype=jnp.int32)
    own_cols = col * TILE + jnp.arange(TILE, dtype=jnp.int32)
    a2_top = jnp.where(own_cols[None, :] > own_rows[:, None], 0.0, a2[:32])
    a2 = jnp.concatenate([a2_top, a2[32:]], 0)

    lines = lax.all_to_all(copies(factor), ("zh", "zl"), 0, 0, tiled=True)[4:]
    both = jnp.concatenate([a2, f2], 0)
    near = lax.ppermute(both, "y", [(2, 1), (3, 0)])
    across = lax.ppermute(both, "y", [(2, 3), (3, 2)])
    sent = near, across, lax.ppermute(both, "y", [(2, 0), (3, 1)])
    last = lines[:, 2].reshape(TILE, TILE)
    low_block, rest = own_pair(last, *over_y(last))
    left1, left2 = (
        lax.ppermute(lines, "x", [(i, (i + s) % 4) for i in range(4)]) for s in (1, 2)
    )
    left3 = lax.ppermute(lines, "x", [(i, (i + 3) % 4) for i in range(4)])
    lefts = (lines, left1, left2, left3)
    odd = lax.axis_index("y") % 2 == 1
    high = jnp.where(odd, rest, low_block)
    pack = jnp.concatenate([jnp.where(odd, low_block, rest), high[64:]], 0)
    packs = (pack, *over_x(pack))
    twins = tuple(swap(p) for p in packs)
    panels = panel_blocks(both, sent, lines)
    adj_panel = jnp.concatenate([p[:288] for p in panels], 1)
    fac_panel = jnp.concatenate([p[288:] for p in panels], 1)

    weights = adj_panel[32:]
    top = jnp.where(low, 1.0, 0.0)
    first = jnp.concatenate([fac_panel[:32] * top, weights], 0)
    second = jnp.concatenate([-adj_panel[:32] * top, fac_panel[32:]], 0)
    steps = jnp.arange(NB, dtype=jnp.int32)
    kept = steps[:, None] >= steps[None, :]
    over_rows = ((0,), (0,))
    middle = -jnp.where(
        kept, close_dot(first, second, over_rows), close_dot(second, first, over_rows)
    )
    f0, f1 = (factor[1:, e].reshape(256, TILE) for e in range(2))
    below = jnp.concatenate([f0, f1, jnp.where(owner, 0.0, f2[32:])], 1)
    outer = close_dot(weights, below, over_rows)
    place = jnp.stack(
        [x, owner.astype(jnp.int32), col * TILE - 512, lax.axis_index("k")]
    ).astype(jnp.int32)
    solved, *parts = solved_parts(place, *packs, *twins, *lefts, outer, middle)
    moved = over_x(tuple(parts[1:]))
    spread = spread_sum(parts[0], *moved)
    share = lax.all_to_all(spread, ("zh", "zl"), 0, 0, tiled=True).sum(axis=0)
    other = lax.ppermute(share, ("zh", "zl"), [(i, 4 + (i + 2) % 4) for i in range(4)])

    update = close_dot(weights, solved).reshape(8, 32, 3, TILE).transpose(0, 2, 1, 3)
    tops = jnp.concatenate([adjoint[0, :2], a2_top[None]], 0)
    new_col = jnp.where(owner, update[:, 2], adjoint[1:, 2] - update[:, 2])
    below = jnp.concatenate([adjoint[1:, :2] - update[:, :2], new_col[:, None]], 1)
    base = jnp.concatenate([tops[None], below], 0)
    end_place = jnp.stack(
        [low.astype(jnp.int32), owner.astype(jnp.int32), row * 32 - col * TILE]
    ).astype(jnp.int32)
    return finished(end_place, base, tops, share, other).transpose(0, 2, 1, 3)


def solution(mesh):
    split_mesh = Mesh(
        mesh.devices.reshape(2, 4, 4, 4, 2), ("zh", "zl", "x", "y", "k")
    )
    placed = P(None, ROW, None, ("y", "k"))
    return jax.shard_map(
        step, mesh=split_mesh, in_specs=(placed, placed), out_specs=placed, check_vma=False
    )
```
